16 devices in a mesh: dp: 2 (over y, z), stage: 8 (over x, core).
Axes of the slice: x: 4, y: 2, z: 1, core: 2. Of those that a mesh axis runs over, the one named last changes fastest.
The devices are a block of a 4x4x8 slice.
Arguments:
- tokens_in: bfloat16 [16, 512, 1024], P('dp'), parts along dimension 0
- targets: bfloat16 [16, 512, 1024], P('dp'), parts along dimension 0
- w_in: bfloat16 [16, 1024, 4096], P('stage')
- w_out: bfloat16 [16, 4096, 1024], P('stage')
- norm_gains: float32 [16, 1024], P('stage')
Outputs:
- output 1: float32 [32, 1024, 4096], P(('dp', 'stage')), parts along dimension 0
- output 2: float32 [32, 4096, 1024], P(('dp', 'stage')), parts along dimension 0
- output 3: float32 [32, 1024], P(('dp', 'stage')), parts along dimension 0
- output 4: float32 [2], P('dp'), parts along dimension 0
There are 2 independent parts. The reference program is written for one: setup_inputs(seed, part) draws one part's arguments, and reference() takes and returns one part's arrays. A program takes and returns all parts, laid end to end along the dimension named above; an argument that names none is the same for every part.
All inputs are finite; a program needn't handle non-finite values.
Results may differ from the reference program's by a relative error of at most 0.00514443.
Values are sent between devices in bfloat16 or wider.
A program may use at most 768 MiB of HBM per device.

```python
import jax
import jax.numpy as jnp
from jax import lax

STAGES = 8
SEGMENT_LAYERS = 1
MICRO_BATCHES = 8
MICRO_TOKENS = 512
D_MODEL = 1024
D_FF = 4096
LAYERS = 2 * STAGES * SEGMENT_LAYERS
EPSILON = 1e-6


def setup_inputs(seed: int = 0, part: int = 0) -> dict:
    base_key = jax.random.key(seed)
    key_list = jax.random.split(base_key, 4)
    data_key = jax.random.fold_in(key_list[0], part)
    key_tokens, key_targets = jax.random.split(data_key)
    shape_act = (MICRO_BATCHES, MICRO_TOKENS, D_MODEL)
    target_scale = (1.0 + 0.5 * LAYERS) ** 0.5
    tokens_in = jax.random.normal(key_tokens, shape_act, jnp.float32)
    targets = target_scale * jax.random.normal(key_targets, shape_act, jnp.float32)
    w_in = jax.random.normal(key_list[1], (LAYERS, D_MODEL, D_FF), jnp.float32) * D_MODEL ** -0.5
    w_out = jax.random.normal(key_list[2], (LAYERS, D_FF, D_MODEL), jnp.float32) * D_FF ** -0.5
    norm_gains = 1.0 + 0.5 * jax.random.normal(key_list[3], (LAYERS, D_MODEL), jnp.float32)
    return {
        'tokens_in': tokens_in.astype(jnp.bfloat16),
        'targets': targets.astype(jnp.bfloat16),
        'w_in': w_in.astype(jnp.bfloat16),
        'w_out': w_out.astype(jnp.bfloat16),
        'norm_gains': norm_gains,
    }


def norm_scale(x_f32, gain_vec):
    inv_rms = lax.rsqrt(jnp.mean(x_f32 * x_f32, axis=-1, keepdims=True) + EPSILON)
    return x_f32 * inv_rms * gain_vec


def layer_forward(x_act, first_w, second_w, gain_vec):
    x_f32 = x_act.astype(jnp.float32)
    normed = norm_scale(x_f32, gain_vec).astype(jnp.bfloat16)
    pre_act = jnp.dot(normed, first_w, preferred_element_type=jnp.float32)
    hidden = jax.nn.gelu(pre_act).astype(jnp.bfloat16)
    out_f32 = jnp.dot(hidden, second_w, preferred_element_type=jnp.float32)
    return (x_f32 + out_f32).astype(jnp.bfloat16)


def layer_backward(x_act, grad_h, first_w, second_w, gain_vec):
    x_f32 = x_act.astype(jnp.float32)
    normed_f32, norm_vjp = jax.vjp(norm_scale, x_f32, gain_vec)
    normed = normed_f32.astype(jnp.bfloat16)
    pre_act = jnp.dot(normed, first_w, preferred_element_type=jnp.float32)
    hidden_f32, gelu_vjp = jax.vjp(jax.nn.gelu, pre_act)
    hidden = hidden_f32.astype(jnp.bfloat16)
    grad_second = jnp.dot(hidden.T, grad_h, preferred_element_type=jnp.float32)
    grad_hidden = jnp.dot(grad_h, second_w.T, preferred_element_type=jnp.float32)
    grad_pre = gelu_vjp(grad_hidden)[0].astype(jnp.bfloat16)
    grad_first = jnp.dot(normed.T, grad_pre, preferred_element_type=jnp.float32)
    grad_normed = jnp.dot(grad_pre, first_w.T, preferred_element_type=jnp.float32)
    grad_x_norm, grad_gain = norm_vjp(grad_normed)
    grad_x = (grad_h.astype(jnp.float32) + grad_x_norm).astype(jnp.bfloat16)
    return grad_x, grad_first, grad_second, grad_gain


def to_exec_order(stored):
    tail_shape = stored.shape[1:]
    blocks = stored.reshape((STAGES, 2, SEGMENT_LAYERS) + tail_shape)
    down_half = blocks[:, 0].reshape((STAGES * SEGMENT_LAYERS,) + tail_shape)
    up_half = blocks[::-1, 1].reshape((STAGES * SEGMENT_LAYERS,) + tail_shape)
    return jnp.concatenate([down_half, up_half], axis=0)


def to_stored_order(in_exec):
    tail_shape = in_exec.shape[1:]
    half_rows = STAGES * SEGMENT_LAYERS
    down_half = in_exec[:half_rows].reshape((STAGES, SEGMENT_LAYERS) + tail_shape)
    up_half = in_exec[half_rows:].reshape((STAGES, SEGMENT_LAYERS) + tail_shape)[::-1]
    return jnp.stack([down_half, up_half], axis=1).reshape((LAYERS,) + tail_shape)


def reference(tokens_in, targets, w_in, w_out, norm_gains):
    first_all = to_exec_order(w_in)
    second_all = to_exec_order(w_out)
    gain_all = to_exec_order(norm_gains)
    seed_scale = 2.0 / (MICRO_BATCHES * MICRO_TOKENS)

    def micro_step(loop_state, micro_pair):
        sum_first, sum_second, sum_gain, sse_total = loop_state
        micro_tokens, micro_targets = micro_pair

        def forward_layer(act_in, layer_weights):
            return layer_forward(act_in, layer_weights[0], layer_weights[1], layer_weights[2]), act_in

        final_act, saved_inputs = lax.scan(forward_layer, micro_tokens, (first_all, second_all, gain_all))
        error_f32 = final_act.astype(jnp.float32) - micro_targets.astype(jnp.float32)
        seed_grad = (error_f32 * seed_scale).astype(jnp.bfloat16)

        def backward_layer(grad_h, layer_data):
            grad_x, grad_first, grad_second, grad_gain = layer_backward(
                layer_data[0], grad_h, layer_data[1], layer_data[2], layer_data[3])
            return grad_x, (grad_first, grad_second, grad_gain)

        _, layer_grads = lax.scan(backward_layer, seed_grad,
                                  (saved_inputs, first_all, second_all, gain_all), reverse=True)
        new_state = (sum_first + layer_grads[0], sum_second + layer_grads[1],
                     sum_gain + layer_grads[2], sse_total + jnp.sum(error_f32 * error_f32))
        return new_state, None

    init_state = (jnp.zeros((LAYERS, D_MODEL, D_FF), jnp.float32),
                  jnp.zeros((LAYERS, D_FF, D_MODEL), jnp.float32),
                  jnp.zeros((LAYERS, D_MODEL), jnp.float32),
                  jnp.zeros((), jnp.float32))
    final_state, _ = lax.scan(micro_step, init_state, (tokens_in, targets))
    loss_value = final_state[3] / (MICRO_BATCHES * MICRO_TOKENS * D_MODEL)
    return (to_stored_order(final_state[0]), to_stored_order(final_state[1]),
            to_stored_order(final_state[2]), loss_value.reshape(1))
```

```python
import functools

import jax
import jax.numpy as jnp
from jax import lax
from jax.experimental import pallas as pl
from jax.experimental.pallas import tpu as pltpu
from jax.sharding import PartitionSpec as P

EPSILON = 1e-6
GRAD_SLOTS = 4
GELU_C = 0.7978845608028654
GELU_A = 0.044715
F32 = jnp.float32
BF16 = jnp.bfloat16
NT = (((1,), (1,)), ((), ()))


def alpha_of(idx):
    return idx + lax.div(idx, 2)


def pipeline_kernel(stages, seed_scale, tokens, targets, w_in, w_out, gains,
                    u_st, da_st, n_st, dh_st, g_st, dgain, loss,
                    wi, wo, xf, bf, gbuf, ubuf, nbuf, obuf, dnbuf, tbuf, sse, sse_in,
                    fsem, bsem, osem, csem, wsem, gsem, usem, nsem, hsem, tsem, lsem, lsend):
    chunks, rows, d_model = tokens.shape
    d_ff = ubuf.shape[1]
    block = min(512, d_ff // 2)
    half = d_model // 2
    me = lax.axis_index('stage')
    last = stages - 1
    alpha = alpha_of(me)
    alpha_max = last + last // 2
    tick_count = 2 * alpha_max + 1 + 2 * (2 * chunks - 1) + 1

    def drain(ref, sem):
        pltpu.make_async_copy(ref, ref, sem).wait()

    barrier = pltpu.get_barrier_semaphore()
    for hop in range(1, stages):
        pl.semaphore_signal(barrier, inc=1, device_id={'stage': lax.rem(me + hop, stages)},
                            device_id_type=pl.DeviceIdType.MESH)
    pl.semaphore_wait(barrier, stages - 1)

    for row in range(2):
        pltpu.make_async_copy(w_in.at[row], wi.at[row], wsem.at[0, row]).start()
        pltpu.make_async_copy(w_out.at[row], wo.at[row], wsem.at[1, row]).start()

    @pl.when(me == 0)
    def _():
        def load_tokens(k, carry):
            pltpu.make_async_copy(tokens.at[k], xf.at[0, k], fsem.at[0, k]).start()
            return carry
        lax.fori_loop(0, chunks, load_tokens, 0)

    dgain[...] = jnp.zeros(dgain.shape, F32)
    sse[...] = jnp.zeros(sse.shape, F32)

    def decode(t):
        par = lax.rem(t + alpha, 2)
        base = alpha + par * (2 * alpha_max + 1 - 2 * alpha)
        step = lax.div(t - base + 8 * stages, 2) - 4 * stages
        return par, step

    def prefetch_slope(t):
        par, step = decode(t)

        @pl.when((step >= chunks) & (step < 2 * chunks))
        def _():
            pltpu.make_async_copy(g_st.at[1 - par, step - chunks], gbuf, gsem).start()

    def free_out(par, step):
        has_out = ((par == 0) & (me < last)) | ((par == 1) & ((me > 0) | (step <= chunks)))

        @pl.when((step > 0) & has_out)
        def _():
            drain(obuf.at[par], osem.at[par])

    def forward(t, par, k):
        x_ref = xf.at[par, k]
        sink = (par == 1) & (me == 0)
        turn = (par == 0) & (me == last)
        free_out(par, k)
        drain(x_ref, fsem.at[par, k])

        @pl.when(sink)
        def _():
            pltpu.make_async_copy(targets.at[k], tbuf, tsem).start()

        x_f32 = x_ref[...].astype(F32)
        inv_rms = lax.rsqrt(jnp.mean(x_f32 * x_f32, axis=-1, keepdims=True) + EPSILON)
        nbuf[...] = (x_f32 * inv_rms * gains[par]).astype(BF16)
        keep_n = pltpu.make_async_copy(nbuf, n_st.at[par, k], nsem)
        keep_n.start()

        @pl.when(k == 0)
        def _():
            drain(wi.at[par], wsem.at[0, par])

        for j in range(d_ff // block):
            cols = slice(j * block, (j + 1) * block)
            pre = jnp.dot(nbuf[...], wi[par, :, cols], preferred_element_type=F32)
            sq = pre * pre
            tanh = jnp.tanh(pre * (GELU_C + (GELU_C * GELU_A) * sq))
            cdf = 0.5 + 0.5 * tanh
            ubuf[:, cols] = (pre * cdf).astype(BF16)
            gbuf[:, cols] = cdf + pre * ((1.0 - tanh * tanh) * (0.5 * GELU_C + (1.5 * GELU_C * GELU_A) * sq))
        keep_u = pltpu.make_async_copy(ubuf, u_st.at[par, k], usem)
        keep_u.start()
        keep_g = pltpu.make_async_copy(gbuf, g_st.at[par, k], gsem)
        keep_g.start()

        @pl.when(k == 0)
        def _():
            drain(wo.at[par], wsem.at[1, par])

        for h in range(2):
            cols = slice(h * half, (h + 1) * half)
            out = x_ref[:, cols].astype(F32) + jnp.dot(ubuf[...], wo[par, :, cols], preferred_element_type=F32)
            obuf[par, :, cols] = out.astype(BF16)
            if h == 0:
                keep_g.wait()
                prefetch_slope(t + 1)

            @pl.when(turn)
            def _():
                pltpu.make_async_copy(obuf.at[0, :, cols], xf.at[1, k, :, cols], fsem.at[1, k]).start()

            @pl.when(jnp.logical_not(turn | sink))
            def _():
                pltpu.make_async_remote_copy(
                    src_ref=obuf.at[par, :, cols], dst_ref=xf.at[par, k, :, cols],
                    send_sem=osem.at[par], recv_sem=fsem.at[par, k],
                    device_id={'stage': me + 1 - 2 * par}, device_id_type=pl.DeviceIdType.MESH).start()

        @pl.when(sink)
        def _():
            drain(tbuf, tsem)
            error = obuf[1].astype(F32) - tbuf[...].astype(F32)
            sse[...] += jnp.sum((error * error).reshape(rows // 8, 8, d_model), axis=0)
            obuf[1] = (error * seed_scale).astype(BF16)
            pltpu.make_async_copy(obuf.at[1], dh_st.at[1, k], osem.at[1]).start()

            @pl.when(k == chunks - 1)
            def _():
                for hop in range(1, stages):
                    pltpu.make_async_remote_copy(
                        src_ref=sse, dst_ref=sse_in, send_sem=lsend.at[hop - 1], recv_sem=lsem,
                        device_id={'stage': hop}, device_id_type=pl.DeviceIdType.MESH).start()

        keep_n.wait()
        keep_u.wait()

    def backward(t, par, step):
        k = step - chunks
        row = 1 - par
        slot = lax.rem(k, GRAD_SLOTS)
        source = (par == 0) & (me == 0)
        sink = (par == 1) & (me == 0)
        turn = (par == 0) & (me == last)
        remote = jnp.logical_not(sink | turn)
        free_out(par, step)

        @pl.when(source & (k == 0))
        def _():
            pltpu.make_async_copy(dh_st.at[1, 0], bf.at[0, 0], bsem.at[0, 0]).start()

        @pl.when(source & (k < chunks - 1))
        def _():
            pltpu.make_async_copy(dh_st.at[1, k + 1], bf.at[0, lax.rem(k + 1, GRAD_SLOTS)],
                                  bsem.at[0, k + 1]).start()

        dh_ref = bf.at[par, slot]
        drain(dh_ref, bsem.at[par, k])
        keep_dh = pltpu.make_async_copy(dh_ref, dh_st.at[row, k], hsem)
        keep_dh.start()
        drain(gbuf, gsem)
        for j in range(d_ff // block):
            cols = slice(j * block, (j + 1) * block)
            d_hidden = lax.dot_general(dh_ref[...], wo[row, cols, :], NT, preferred_element_type=F32)
            ubuf[:, cols] = (d_hidden * gbuf[:, cols]).astype(BF16)
        prefetch_slope(t + 1)
        keep_da = pltpu.make_async_copy(ubuf, da_st.at[row, k], usem)
        keep_da.start()
        for h in range(2):
            cols = slice(h * half, (h + 1) * half)
            dnbuf[:, cols] = lax.dot_general(ubuf[...], wi[row, cols, :], NT, preferred_element_type=F32)
        x_f32 = xf[row, k].astype(F32)
        d_normed = dnbuf[...]
        inv_rms = lax.rsqrt(jnp.mean(x_f32 * x_f32, axis=-1, keepdims=True) + EPSILON)
        x_hat = x_f32 * inv_rms
        dgain[row] += jnp.sum((d_normed * x_hat).reshape(rows // 8, 8, d_model), axis=0)
        scaled = d_normed * gains[row]
        proj = jnp.mean(scaled * x_hat, axis=-1, keepdims=True)
        grad_x = dh_ref[...].astype(F32) + inv_rms * (scaled - x_hat * proj)
        obuf[par] = grad_x.astype(BF16)

        @pl.when(remote)
        def _():
            @pl.when(k >= GRAD_SLOTS)
            def _():
                pl.semaphore_wait(csem.at[par], 1)
            pltpu.make_async_remote_copy(
                src_ref=obuf.at[par], dst_ref=bf.at[par, slot],
                send_sem=osem.at[par], recv_sem=bsem.at[par, k],
                device_id={'stage': me + 1 - 2 * par}, device_id_type=pl.DeviceIdType.MESH).start()

        @pl.when(turn)
        def _():
            pltpu.make_async_copy(obuf.at[0], bf.at[1, slot], bsem.at[1, k]).start()

        keep_dh.wait()
        keep_da.wait()
        from_peer = ((par == 0) & (me > 0)) | ((par == 1) & (me < last))

        @pl.when(from_peer & (k < chunks - GRAD_SLOTS))
        def _():
            pl.semaphore_signal(csem.at[par], inc=1, device_id={'stage': me - 1 + 2 * par},
                                device_id_type=pl.DeviceIdType.MESH)

    def tick(t, carry):
        par, step = decode(t)
        is_fwd = (step >= 0) & (step < chunks)
        is_bwd = (step >= chunks) & (step < 2 * chunks)

        @pl.when(is_fwd)
        def _():
            forward(t, par, step)

        @pl.when(is_bwd)
        def _():
            backward(t, par, step)

        @pl.when(jnp.logical_not(is_fwd | is_bwd))
        def _():
            prefetch_slope(t + 1)

        return carry

    lax.fori_loop(0, tick_count, tick, 0)

    for par in range(2):
        has_out = (me < last) if par == 0 else (me > 0)

        @pl.when(has_out)
        def _():
            drain(obuf.at[par], osem.at[par])

    @pl.when(me == 0)
    def _():
        for hop in range(1, stages):
            drain(sse, lsend.at[hop - 1])
        loss[...] = sse[...]

    @pl.when(me > 0)
    def _():
        drain(sse_in, lsem)
        loss[...] = sse_in[...]


def run_pipeline(stages, seed_scale, tokens, targets, w_in, w_out, gains):
    chunks, rows, d_model = tokens.shape
    d_ff = w_in.shape[2]
    hbm = pl.BlockSpec(memory_space=pl.ANY)
    vmem = pl.BlockSpec(memory_space=pltpu.VMEM)
    out_shape = (
        jax.ShapeDtypeStruct((2, chunks, rows, d_ff), BF16),
        jax.ShapeDtypeStruct((2, chunks, rows, d_ff), BF16),
        jax.ShapeDtypeStruct((2, chunks, rows, d_model), BF16),
        jax.ShapeDtypeStruct((2, chunks, rows, d_model), BF16),
        jax.ShapeDtypeStruct((2, chunks, rows, d_ff), F32),
        jax.ShapeDtypeStruct((2, 8, d_model), F32),
        jax.ShapeDtypeStruct((8, d_model), F32),
    )
    dma = pltpu.SemaphoreType.DMA
    scratch = [
        pltpu.VMEM((2, d_model, d_ff), BF16),
        pltpu.VMEM((2, d_ff, d_model), BF16),
        pltpu.VMEM((2, chunks, rows, d_model), BF16),
        pltpu.VMEM((2, GRAD_SLOTS, rows, d_model), BF16),
        pltpu.VMEM((rows, d_ff), F32),
        pltpu.VMEM((rows, d_ff), BF16),
        pltpu.VMEM((rows, d_model), BF16),
        pltpu.VMEM((2, rows, d_model), BF16),
        pltpu.VMEM((rows, d_model), F32),
        pltpu.VMEM((rows, d_model), BF16),
        pltpu.VMEM((8, d_model), F32),
        pltpu.VMEM((8, d_model), F32),
        dma((2, chunks)), dma((2, chunks)), dma((2,)), pltpu.SemaphoreType.REGULAR((2,)), dma((2, 2)),
        dma, dma, dma, dma, dma, dma, dma((stages - 1,)),
    ]
    flops = 2 * chunks * 8 * rows * d_model * d_ff
    return pl.pallas_call(
        functools.partial(pipeline_kernel, stages, seed_scale),
        out_shape=out_shape,
        in_specs=[hbm, hbm, hbm, hbm, vmem],
        out_specs=(hbm, hbm, hbm, hbm, hbm, vmem, vmem),
        scratch_shapes=scratch,
        compiler_params=pltpu.CompilerParams(
            collective_id=0, has_side_effects=True, vmem_limit_bytes=67043328),
        cost_estimate=pl.CostEstimate(flops=flops, bytes_accessed=16 * chunks * rows * d_ff, transcendentals=0),
        name='pipeline',
    )(tokens, targets, w_in, w_out, gains)


def solution(mesh):
    stages = mesh.shape['stage']

    def device_step(tokens, targets, w_in, w_out, norm_gains):
        micro_count, tokens_mb, d_model = tokens.shape
        d_ff = w_in.shape[2]
        total = micro_count * tokens_mb
        rows = tokens_mb // 2
        chunked = (total // rows, rows, d_model)
        u_st, da_st, n_st, dh_st, _, dgain, sse = run_pipeline(
            stages, 2.0 / total, tokens.reshape(chunked), targets.reshape(chunked),
            w_in, w_out, norm_gains.reshape(2, 1, d_model))
        u_all = u_st.reshape(2, total, d_ff)
        da_all = da_st.reshape(2, total, d_ff)
        n_all = n_st.reshape(2, total, d_model)
        dh_all = dh_st.reshape(2, total, d_model)
        grad_w_in = jnp.einsum('ltd,ltf->ldf', n_all, da_all, preferred_element_type=F32)
        grad_w_out = jnp.einsum('ltf,ltd->lfd', u_all, dh_all, preferred_element_type=F32)
        grad_gains = jnp.sum(dgain, axis=1)
        loss_value = jnp.sum(sse) / (total * d_model)
        return grad_w_in, grad_w_out, grad_gains, loss_value.reshape(1)

    block_spec = P(('dp', 'stage'))
    return jax.shard_map(device_step, mesh=mesh,
                         in_specs=(P('dp'), P('dp'), P('stage'), P('stage'), P('stage')),
                         out_specs=(block_spec, block_spec, block_spec, P('dp')),
                         check_vma=False)
```

```python
import functools

import jax
import jax.numpy as jnp
from jax import lax
from jax.experimental import pallas as pl
from jax.experimental.pallas import tpu as pltpu
from jax.sharding import PartitionSpec as P

EPSILON = 1e-6
GRAD_SLOTS = 4
HOP_TICKS = 2
TURN_TICKS = 2
GAP = 1
BLOCK = 256
SLAB = 32
KEPT_SLOPE = 4
GELU_C = 0.7978845608028654
GELU_A = 0.044715
F32 = jnp.float32
BF16 = jnp.bfloat16
NT = (((1,), (1,)), ((), ()))


def slope_of(pre):
    sq = pre * pre
    cdf = 0.5 + 0.5 * jnp.tanh(pre * (GELU_C + (GELU_C * GELU_A) * sq))
    hidden = pre * cdf
    return hidden, cdf + (hidden * (1.0 - cdf)) * (2.0 * GELU_C + (6.0 * GELU_C * GELU_A) * sq)


def pipeline_kernel(stages, seed_scale, tokens, targets, w_in, w_out, gains,
                    u_st, da_st, n_st, dh_st, g_st, dgain, loss,
                    wi, wo, xf, bf, gbuf, ubuf, nbuf, obuf, dnbuf, tbuf, sse, sse_in,
                    fsem, bsem, osem, csem, wsem, gsem, usem, nsem, hsem, tsem, lsem, lsend):
    chunks, rows, d_model = tokens.shape
    d_ff = ubuf.shape[1]
    block = min(BLOCK, d_ff // 2)
    blocks = d_ff // block
    slab = min(SLAB, rows // 2)
    wide = d_ff // 2
    half = d_model // 2
    me = lax.axis_index('stage')
    last = stages - 1
    alpha = HOP_TICKS * me
    up_base = 2 * HOP_TICKS * last + TURN_TICKS + 1
    tick_count = up_base + 2 * (2 * chunks - 1 + GAP) + 1
    bwd_from = chunks + GAP

    def drain(ref, sem):
        pltpu.make_async_copy(ref, ref, sem).wait()

    barrier = pltpu.get_barrier_semaphore()
    for hop in range(1, stages):
        pl.semaphore_signal(barrier, inc=1, device_id={'stage': lax.rem(me + hop, stages)},
                            device_id_type=pl.DeviceIdType.MESH)
    pl.semaphore_wait(barrier, stages - 1)

    def load_weights(row):
        pltpu.make_async_copy(w_in.at[row], wi.at[row], wsem.at[0, row]).start()
        pltpu.make_async_copy(w_out.at[row], wo.at[row], wsem.at[1, row]).start()

    def load_tokens(k, carry):
        pltpu.make_async_copy(tokens.at[k], xf.at[0, k], fsem.at[0, k]).start()
        return carry

    @pl.when(me == 0)
    def _():
        load_tokens(0, 0)

    load_weights(0)

    dgain[...] = jnp.zeros(dgain.shape, F32)
    sse[...] = jnp.zeros(sse.shape, F32)

    def decode(t):
        par = lax.rem(t + alpha, 2)
        base = alpha + par * (up_base - 2 * alpha)
        step = lax.div(t - base + 8 * stages, 2) - 4 * stages
        return par, step

    def prefetch_slope(t, h):
        par, step = decode(t)
        cols = slice(h * wide, (h + 1) * wide)

        @pl.when((step >= bwd_from) & (step < bwd_from + chunks))
        def _():
            pltpu.make_async_copy(g_st.at[1 - par, step - bwd_from, :, cols], gbuf.at[:, cols], gsem.at[h]).start()

    def slope_ready(h):
        cols = slice(h * wide, (h + 1) * wide)
        drain(gbuf.at[:, cols], gsem.at[h])

    def forward(t, par, k):
        x_ref = xf.at[par, k]
        sink = (par == 1) & (me == 0)
        turn = (par == 0) & (me == last)
        @pl.when((k > 0) & (((par == 0) & (me < last)) | ((par == 1) & (me > 0))))
        def _():
            drain(obuf.at[par], osem.at[par])

        @pl.when((par == 0) | (me < last))
        def _():
            drain(x_ref, fsem.at[par, k])

        @pl.when(sink)
        def _():
            pltpu.make_async_copy(targets.at[k], tbuf, tsem).start()

        for at in range(0, rows, slab):
            span = slice(at, at + slab)
            x_f32 = x_ref[span, :].astype(F32)
            inv_rms = lax.rsqrt(jnp.mean(x_f32 * x_f32, axis=-1, keepdims=True) + EPSILON)
            nbuf[span, :] = (x_f32 * inv_rms * gains[par]).astype(BF16)
        keep_n = pltpu.make_async_copy(nbuf, n_st.at[par, k], nsem)
        keep_n.start()

        @pl.when(k == 0)
        def _():
            drain(wi.at[par], wsem.at[0, par])
            drain(wo.at[par], wsem.at[1, par])

        @pl.when((k == 0) & (par == 0))
        def _():
            load_weights(1)

            @pl.when(me == 0)
            def _():
                lax.fori_loop(1, chunks, load_tokens, 0)

        def first_dot(j):
            return jnp.dot(nbuf[...], wi[par, :, j * block:(j + 1) * block], preferred_element_type=F32)

        def activate(j, pre):
            cols = slice(j * block, (j + 1) * block)
            if j * 8 < KEPT_SLOPE * blocks:
                hidden, kept = slope_of(pre)
            else:
                sq = pre * pre
                hidden = pre * (0.5 + 0.5 * jnp.tanh(pre * (GELU_C + (GELU_C * GELU_A) * sq)))
                kept = pre
            ubuf[:, cols] = hidden.astype(BF16)
            gbuf[:, cols] = kept

        def second_dot(j):
            cols = slice(j * block, (j + 1) * block)
            part = jnp.dot(ubuf[:, cols], wo[par, cols, :half], preferred_element_type=F32)
            base = x_ref[:, :half].astype(F32) if j == 0 else dnbuf[:, :half]
            total = base + part
            if j == blocks - 1:
                obuf[par, :, :half] = total.astype(BF16)
            else:
                dnbuf[:, :half] = total

        def send_half(cols):
            @pl.when(turn)
            def _():
                xf[1, k, :, cols] = obuf[0, :, cols]

            @pl.when(jnp.logical_not(turn | sink))
            def _():
                pltpu.make_async_remote_copy(
                    src_ref=obuf.at[par, :, cols], dst_ref=xf.at[par, k, :, cols],
                    send_sem=osem.at[par], recv_sem=fsem.at[par, k],
                    device_id={'stage': me + 1 - 2 * par}, device_id_type=pl.DeviceIdType.MESH).start()

        def keep_slope(h):
            cols = slice(h * wide, (h + 1) * wide)
            pltpu.make_async_copy(gbuf.at[:, cols], g_st.at[par, k, :, cols], gsem.at[h]).start()
            pltpu.make_async_copy(ubuf.at[:, cols], u_st.at[par, k, :, cols], usem).start()

        pre = first_dot(0)
        for j in range(blocks):
            activate(j, pre)
            if j + 1 < blocks:
                pre = first_dot(j + 1)
            second_dot(j)
            if j == blocks // 2 - 1:
                keep_slope(0)
        send_half(slice(0, half))
        keep_slope(1)
        slope_ready(0)
        prefetch_slope(t + 1, 0)
        out = x_ref[:, half:].astype(F32) + jnp.dot(ubuf[...], wo[par, :, half:], preferred_element_type=F32)
        obuf[par, :, half:] = out.astype(BF16)
        send_half(slice(half, d_model))
        slope_ready(1)
        prefetch_slope(t + 1, 1)

        @pl.when(sink)
        def _():
            drain(tbuf, tsem)
            error = obuf[1].astype(F32) - tbuf[...].astype(F32)
            sse[...] += jnp.sum((error * error).reshape(rows // 8, 8, d_model), axis=0)
            bf[0, lax.rem(k, GRAD_SLOTS)] = (error * seed_scale).astype(BF16)

            @pl.when(k == chunks - 1)
            def _():
                for hop in range(1, stages):
                    pltpu.make_async_remote_copy(
                        src_ref=sse, dst_ref=sse_in, send_sem=lsend.at[hop - 1], recv_sem=lsem,
                        device_id={'stage': hop}, device_id_type=pl.DeviceIdType.MESH).start()

        keep_n.wait()
        drain(ubuf, usem)

    def backward(t, par, step):
        k = step - bwd_from
        row = 1 - par
        slot = lax.rem(k, GRAD_SLOTS)
        from_peer = ((par == 0) & (me > 0)) | ((par == 1) & (me < last))
        sink = (par == 1) & (me == 0)
        turn = (par == 0) & (me == last)
        remote = jnp.logical_not(sink | turn)
        @pl.when(((par == 0) & (me < last)) | ((par == 1) & (me > 0)))
        def _():
            drain(obuf.at[par], osem.at[par])

        dh_ref = bf.at[par, slot]

        @pl.when(from_peer)
        def _():
            drain(dh_ref, bsem.at[par, k])

        keep_dh = pltpu.make_async_copy(dh_ref, dh_st.at[row, k], hsem)
        keep_dh.start()
        for j in range(blocks):
            if j == 0:
                slope_ready(0)
            if j == blocks // 2:
                slope_ready(1)
            cols = slice(j * block, (j + 1) * block)
            d_hidden = lax.dot_general(dh_ref[...], wo[row, cols, :], NT, preferred_element_type=F32)
            kept = gbuf[:, cols]
            slope = kept if j * 8 < KEPT_SLOPE * blocks else slope_of(kept)[1]
            ubuf[:, cols] = (d_hidden * slope).astype(BF16)
        prefetch_slope(t + 1, 0)
        prefetch_slope(t + 1, 1)
        keep_da = pltpu.make_async_copy(ubuf, da_st.at[row, k], usem)
        keep_da.start()
        for h in range(2):
            cols = slice(h * half, (h + 1) * half)
            dnbuf[:, cols] = lax.dot_general(ubuf[...], wi[row, cols, :], NT, preferred_element_type=F32)

        @pl.when(remote & (k >= GRAD_SLOTS))
        def _():
            pl.semaphore_wait(csem.at[par], 1)

        gain_sum = dgain[row]
        for at in range(0, rows, slab):
            span = slice(at, at + slab)
            x_f32 = xf[row, k, span, :].astype(F32)
            d_normed = dnbuf[span, :]
            inv_rms = lax.rsqrt(jnp.mean(x_f32 * x_f32, axis=-1, keepdims=True) + EPSILON)
            x_hat = x_f32 * inv_rms
            gain_sum = gain_sum + jnp.sum((d_normed * x_hat).reshape(slab // 8, 8, d_model), axis=0)
            scaled = d_normed * gains[row]
            proj = jnp.mean(scaled * x_hat, axis=-1, keepdims=True)
            grad_x = dh_ref[span, :].astype(F32) + inv_rms * (scaled - x_hat * proj)
            obuf[par, span, :] = grad_x.astype(BF16)
            if (at + slab) % (rows // 2) == 0:
                part = slice(at + slab - rows // 2, at + slab)

                @pl.when(remote)
                def _():
                    pltpu.make_async_remote_copy(
                        src_ref=obuf.at[par, part, :], dst_ref=bf.at[par, slot, part, :],
                        send_sem=osem.at[par], recv_sem=bsem.at[par, k],
                        device_id={'stage': me + 1 - 2 * par}, device_id_type=pl.DeviceIdType.MESH).start()
        dgain[row] = gain_sum

        @pl.when(turn)
        def _():
            bf[1, slot] = obuf[0]

        keep_dh.wait()
        keep_da.wait()
        @pl.when(from_peer & (k < chunks - GRAD_SLOTS))
        def _():
            pl.semaphore_signal(csem.at[par], inc=1, device_id={'stage': me - 1 + 2 * par},
                                device_id_type=pl.DeviceIdType.MESH)

    def tick(t, carry):
        par, step = decode(t)
        is_fwd = (step >= 0) & (step < chunks)
        is_bwd = (step >= bwd_from) & (step < bwd_from + chunks)

        @pl.when(is_fwd)
        def _():
            forward(t, par, step)

        @pl.when(is_bwd)
        def _():
            backward(t, par, step)

        @pl.when(jnp.logical_not(is_fwd | is_bwd))
        def _():
            prefetch_slope(t + 1, 0)
            prefetch_slope(t + 1, 1)

        return carry

    lax.fori_loop(0, tick_count, tick, 0)

    for par in range(2):
        has_out = (me < last) if par == 0 else (me > 0)

        @pl.when(has_out)
        def _():
            drain(obuf.at[par], osem.at[par])

    @pl.when(me == 0)
    def _():
        for hop in range(1, stages):
            drain(sse, lsend.at[hop - 1])
        loss[...] = sse[...]

    @pl.when(me > 0)
    def _():
        drain(sse_in, lsem)
        loss[...] = sse_in[...]


def run_pipeline(stages, seed_scale, tokens, targets, w_in, w_out, gains):
    chunks, rows, d_model = tokens.shape
    d_ff = w_in.shape[2]
    hbm = pl.BlockSpec(memory_space=pl.ANY)
    vmem = pl.BlockSpec(memory_space=pltpu.VMEM)
    out_shape = (
        jax.ShapeDtypeStruct((2, chunks, rows, d_ff), BF16),
        jax.ShapeDtypeStruct((2, chunks, rows, d_ff), BF16),
        jax.ShapeDtypeStruct((2, chunks, rows, d_model), BF16),
        jax.ShapeDtypeStruct((2, chunks, rows, d_model), BF16),
        jax.ShapeDtypeStruct((2, chunks, rows, d_ff), F32),
        jax.ShapeDtypeStruct((2, 8, d_model), F32),
        jax.ShapeDtypeStruct((8, d_model), F32),
    )
    dma = pltpu.SemaphoreType.DMA
    scratch = [
        pltpu.VMEM((2, d_model, d_ff), BF16),
        pltpu.VMEM((2, d_ff, d_model), BF16),
        pltpu.VMEM((2, chunks, rows, d_model), BF16),
        pltpu.VMEM((2, GRAD_SLOTS, rows, d_model), BF16),
        pltpu.VMEM((rows, d_ff), F32),
        pltpu.VMEM((rows, d_ff), BF16),
        pltpu.VMEM((rows, d_model), BF16),
        pltpu.VMEM((2, rows, d_model), BF16),
        pltpu.VMEM((rows, d_model), F32),
        pltpu.VMEM((rows, d_model), BF16),
        pltpu.VMEM((8, d_model), F32),
        pltpu.VMEM((8, d_model), F32),
        dma((2, chunks)), dma((2, chunks)), dma((2,)), pltpu.SemaphoreType.REGULAR((2,)), dma((2, 2)),
        dma((2,)), dma, dma, dma, dma, dma, dma((stages - 1,)),
    ]
    flops = 2 * chunks * 8 * rows * d_model * d_ff
    return pl.pallas_call(
        functools.partial(pipeline_kernel, stages, seed_scale),
        out_shape=out_shape,
        in_specs=[hbm, hbm, hbm, hbm, vmem],
        out_specs=(hbm, hbm, hbm, hbm, hbm, vmem, vmem),
        scratch_shapes=scratch,
        compiler_params=pltpu.CompilerParams(
            collective_id=0, has_side_effects=True, vmem_limit_bytes=67043328),
        cost_estimate=pl.CostEstimate(flops=flops, bytes_accessed=16 * chunks * rows * d_ff, transcendentals=0),
        name='pipeline',
    )(tokens, targets, w_in, w_out, gains)


def solution(mesh):
    stages = mesh.shape['stage']

    def device_step(tokens, targets, w_in, w_out, norm_gains):
        micro_count, tokens_mb, d_model = tokens.shape
        d_ff = w_in.shape[2]
        total = micro_count * tokens_mb
        rows = tokens_mb // 2
        chunked = (total // rows, rows, d_model)
        u_st, da_st, n_st, dh_st, _, dgain, sse = run_pipeline(
            stages, 2.0 / total, tokens.reshape(chunked), targets.reshape(chunked),
            w_in, w_out, norm_gains.reshape(2, 1, d_model))
        u_all = u_st.reshape(2, total, d_ff)
        da_all = da_st.reshape(2, total, d_ff)
        n_all = n_st.reshape(2, total, d_model)
        dh_all = dh_st.reshape(2, total, d_model)
        grad_w_in = jnp.einsum('ltd,ltf->ldf', n_all, da_all, preferred_element_type=F32)
        grad_w_out = jnp.einsum('ltf,ltd->lfd', u_all, dh_all, preferred_element_type=F32)
        grad_gains = jnp.sum(dgain, axis=1)
        loss_value = jnp.sum(sse) / (total * d_model)
        return grad_w_in, grad_w_out, grad_gains, loss_value.reshape(1)

    block_spec = P(('dp', 'stage'))
    return jax.shard_map(device_step, mesh=mesh,
                         in_specs=(P('dp'), P('dp'), P('stage'), P('stage'), P('stage')),
                         out_specs=(block_spec, block_spec, block_spec, P('dp')),
                         check_vma=False)
```
